16 devices in a mesh: dp: 1, tp: 16 (over x, y, z, core).
Axes of the slice: x: 2, y: 2, z: 2, core: 2. Of those that a mesh axis runs over, the one named last changes fastest.
Arguments:
- x: bfloat16 [2048, 1024], P('dp')
- gain: bfloat16 [1024], replicated
- wq: bfloat16 [1024, 16384], P(None, 'tp')
- wk: bfloat16 [1024, 16384], P(None, 'tp')
- wv: bfloat16 [1024, 16384], P(None, 'tp')
- wo: bfloat16 [16384, 1024], P('tp')
Outputs:
- output: bfloat16 [2048, 1024], P('dp')
All inputs are finite; a program needn't handle non-finite values.
Results may differ from the reference program's by a relative error of at most 0.012.
Values are sent between devices in bfloat16 or wider.
A program may use at most 2 GiB of HBM per device.

```python
import jax
import jax.numpy as jnp
from jax import lax

ROWS = 2048
D = 1024
HEADS = 128
KV_HEADS = 128
HEAD = 128
THETA = 10000


def setup_inputs(seed: int = 0, part: int = 0) -> dict:
    kx, kn, kq, kk, kv, ko = jax.random.split(jax.random.key(seed), 6)

    def weights(key, rows, columns):
        return jax.random.normal(key, (rows, columns), jnp.float32) * rows**-0.5

    drawn = {
        "x": jax.random.normal(jax.random.fold_in(kx, part), (ROWS, D), jnp.float32),
        "gain": 1 + 0.1 * jax.random.normal(kn, (D,), jnp.float32),
        "wq": 2 * weights(kq, D, HEADS * HEAD),
        "wk": 2 * weights(kk, D, KV_HEADS * HEAD),
        "wv": 4 * weights(kv, D, KV_HEADS * HEAD),
        "wo": weights(ko, HEADS * HEAD, D),
    }
    return {k: v.astype(jnp.bfloat16) for k, v in drawn.items()}


def normed(x, gain):
    wide = x.astype(jnp.float32)
    scale = lax.rsqrt(jnp.mean(wide * wide, -1, keepdims=True) + 1e-6)
    return (wide * scale * gain.astype(jnp.float32)).astype(jnp.bfloat16)


def turned(t, place, theta):
    half = t.shape[-1] // 2
    angle = place.astype(jnp.float32)[:, None] * theta ** (-jnp.arange(half, dtype=jnp.float32) / half)
    cos, sin = jnp.cos(angle)[:, None], jnp.sin(angle)[:, None]
    a, b = t[..., :half].astype(jnp.float32), t[..., half:].astype(jnp.float32)
    return jnp.concatenate([a * cos - b * sin, b * cos + a * sin], -1).astype(jnp.bfloat16)


def matmul(a, w):
    return jnp.dot(a, w, preferred_element_type=jnp.float32).astype(jnp.bfloat16)


def einsum(form, a, b):
    return jnp.einsum(form, a.astype(jnp.float32), b.astype(jnp.float32))


def attention(q, k, v):
    scores = einsum("tgsd,ugd->gstu", q, k) * q.shape[-1] ** -0.5
    token = jnp.arange(q.shape[0])
    scores = jnp.where(token[:, None] >= token, scores, -jnp.inf)
    weights = jax.nn.softmax(scores, -1).astype(jnp.bfloat16)
    return einsum("gstu,ugd->tgsd", weights, v).astype(jnp.bfloat16)


def reference(x, gain, wq, wk, wv, wo):
    a, place = normed(x, gain), jnp.arange(ROWS)
    q = turned(matmul(a, wq).reshape(ROWS, HEADS, HEAD), place, THETA).reshape(ROWS, KV_HEADS, -1, HEAD)
    k = turned(matmul(a, wk).reshape(ROWS, KV_HEADS, HEAD), place, THETA)
    v = matmul(a, wv).reshape(ROWS, KV_HEADS, HEAD)
    seen = attention(q, k, v).reshape(ROWS, HEADS * HEAD)
    return (x.astype(jnp.float32) + jnp.dot(seen, wo, preferred_element_type=jnp.float32)).astype(jnp.bfloat16)
```

```python
import functools

import jax
import jax.numpy as jnp
import numpy as np
from jax import lax
from jax.experimental import pallas as pl
from jax.experimental.pallas import tpu as pltpu
from jax.sharding import PartitionSpec as P

HEAD = 128
THETA = 10000
LOG2E = 1.4426950408889634
ROWS, D = 2048, 1024
HEADS = 8
PAIRS = HEADS // 2
QB = 256
NB = ROWS // QB
PB = 512
KC = 256
WIDE = HEAD + 16
HALF = QB // 2
PART = HALF // 8
CHIPS = 8
SCALE = HEAD**-0.5
F32, BF16 = jnp.float32, jnp.bfloat16


def dot(a, b, ca=1, cb=0):
    return lax.dot_general(a, b, (((ca,), (cb,)), ((), ())), preferred_element_type=F32)


def rotary_tables():
    half = HEAD // 2
    rate = THETA ** (-np.arange(half) / half)

    def both(place):
        angle = place[:, None] * rate
        cos, sin = np.cos(angle), np.sin(angle)
        return np.concatenate([cos, cos], 1).astype(np.float32), np.concatenate([-sin, sin], 1).astype(np.float32)

    near = both(np.arange(PB, dtype=np.float64))
    far = both(np.arange(ROWS // PB, dtype=np.float64) * PB)
    far = tuple(np.concatenate([f, np.zeros((8 - f.shape[0], HEAD), np.float32)]) for f in far)
    return np.stack(near), np.stack(far)


def kernel(x_hbm, gain_ref, near_hbm, far_ref, wq_hbm, wk_hbm, wv_hbm, wo_hbm, y_ref,
           x_v, near_v, wq_v, wk_v, wv_v, wo_v, h_v, cos_v, sin_v, q_v, k_v, vt_v, s0_v, s1_v, o_v, acc_v,
           pair_send, pair_recv, rs_send, rs_recv, own_v,
           in_sem, pair_ss, pair_rs, rs_ss, rs_rs, ag_ss, ag_rs, fw_ss, fw_rs):
    dp, me = lax.axis_index("dp"), lax.axis_index("tp")
    core = lax.rem(me, 2)
    chip = lax.div(me, 2)
    bits = [lax.rem(lax.div(chip, 4), 2), lax.rem(lax.div(chip, 2), 2), lax.rem(chip, 2)]

    def other(k):
        at = [1 - b if (k >> (2 - i)) & 1 else b for i, b in enumerate(bits)]
        return at[0] * 4 + at[1] * 2 + at[2]

    def device(chip_, core_):
        return {"tp": chip_ * 2 + core_}

    partner = device(chip, 1 - core)
    peers = [device(other(k), core) for k in range(1, CHIPS)]

    def fetch(i, src, dst):
        return pltpu.make_async_copy(src, dst, in_sem.at[i])

    loads = {}
    for p in range(ROWS // PB):
        loads["x", p] = fetch(p, x_hbm.at[pl.ds(p * PB, PB), :], x_v.at[pl.ds(p * PB, PB), :])
    loads["near"] = fetch(4, near_hbm, near_v)
    for c in range(PAIRS):
        for n, (name, src, dst) in enumerate((("q", wq_hbm, wq_v), ("k", wk_hbm, wk_v), ("v", wv_hbm, wv_v))):
            loads[name, c] = fetch(5 + 3 * c + n, src.at[:, pl.ds(c * 256, 256)], dst.at[c])
    loads["wo"] = fetch(17, wo_hbm, wo_v)
    order = [("x", 0), "near"] + [(n, c) for c in range(PAIRS) for n in "qkv"] + [("x", 1), "wo", ("x", 2), ("x", 3)]
    for key in order:
        loads[key].start()

    barrier = pltpu.get_barrier_semaphore()
    for peer in [partner] + peers:
        pl.semaphore_signal(barrier, inc=1, device_id=peer, device_id_type=pl.DeviceIdType.MESH)

    for h in range(HEADS):
        vt_v[h, HEAD:, :] = jnp.ones((WIDE - HEAD, ROWS), BF16)

    def project(p):
        rows = pl.ds(p * PB, PB)
        loads["x", p].wait()
        wide = x_v[rows, :].astype(F32)
        scale = lax.rsqrt(jnp.mean(wide * wide, -1, keepdims=True) + 1e-6)
        h_v[...] = (wide * scale * gain_ref[...].astype(F32)).astype(BF16)
        if p == 0:
            loads["near"].wait()
            cos_v[...] = near_v[0]
            sin_v[...] = near_v[1]
        else:
            cf, sf = far_ref[0, p : p + 1, :], far_ref[1, p : p + 1, :]
            cn, sn = near_v[0], near_v[1]
            cos_v[...] = cn * cf - sn * sf
            sin_v[...] = sn * cf + cn * sf

        def turned(t):
            t = t.astype(BF16).astype(F32)
            return (t * cos_v[...] + pltpu.roll(t, HEAD // 2, 1) * sin_v[...]).astype(BF16)

        def body(c, _):
            if p == 0:
                for n, (src, dst) in enumerate(((wq_hbm, wq_v), (wk_hbm, wk_v), (wv_hbm, wv_v))):
                    pltpu.make_async_copy(src.at[:, pl.ds(0, 256)], dst.at[c], in_sem.at[5 + 3 * c + n]).wait()
            a = h_v[...]
            tq = dot(a, wq_v[c])
            tk = dot(a, wk_v[c])
            tv = dot(a, wv_v[c])
            for n in range(2):
                lanes = slice(n * HEAD, (n + 1) * HEAD)
                q_v[2 * c + n, rows, :] = turned(tq[:, lanes])
                k_v[2 * c + n, rows, :] = turned(tk[:, lanes])
                vt_v[2 * c + n, :HEAD, rows] = tv[:, lanes].astype(BF16).T
            return 0

        lax.fori_loop(0, PAIRS, body, 0)

    e = SCALE * LOG2E

    def attention(b, hook):
        rows = pl.ds(b * QB, QB)
        n = b + 1

        def score(h, c, s_v, top):
            s = dot(k_v[h, pl.ds(c * KC, KC), :], q_v[h, rows, :], 1, 1)
            if c == b:
                ok = lax.broadcasted_iota(jnp.int32, (KC, QB), 0) <= lax.broadcasted_iota(jnp.int32, (KC, QB), 1)
                s = jnp.where(ok, s, -jnp.inf)
            s_v[pl.ds(c * KC, KC), :] = s
            m = s.reshape(KC // 8, 8, QB).max(axis=0)
            return m if top is None else jnp.maximum(top, m)

        def mixed(h, c, s_v, top, acc):
            w = jnp.exp2((s_v[pl.ds(c * KC, KC), :] - top) * e).astype(BF16)
            m = dot(vt_v[h, :, pl.ds(c * KC, KC)], w)
            return m if acc is None else acc + m

        def step(h, s_v, top, h_next, s_next):
            acc = new = None
            top = top.max(axis=0, keepdims=True)
            for c in range(n):
                if h_next is not None:
                    new = score(h_next, c, s_next, new)
                acc = mixed(h, c, s_v, top, acc)
            out = acc[:HEAD, :] * (1 / acc[HEAD : HEAD + 1, :])
            return out.T.astype(BF16), new

        def pair(i, top, last):
            out, top = step(2 * i, s0_v, top, 2 * i + 1, s1_v)
            o_v[i, :, :HEAD] = out
            out, top = step(2 * i + 1, s1_v, top, None if last else 2 * i + 2, s0_v)
            o_v[i, :, HEAD:] = out
            return top

        top = None
        for c in range(n):
            top = score(0, c, s0_v, top)

        def body(i, top):
            @pl.when(i == 1)
            def _():
                hook()

            return pair(i, top, False)

        top = lax.fori_loop(0, PAIRS - 1, body, top)
        pair(PAIRS - 1, top, True)

    def remote(src, dst, ss, rs, dev):
        return pltpu.make_async_remote_copy(src_ref=src, dst_ref=dst, send_sem=ss, recv_sem=rs, device_id=dev,
                                            device_id_type=pl.DeviceIdType.MESH)

    mine = pl.multiple_of(core * HALF, HALF)
    theirs = pl.multiple_of((1 - core) * HALF, HALF)

    def pair_copy(b):
        return remote(pair_send.at[b], pair_recv.at[b], pair_ss.at[b], pair_rs.at[b], partner)

    def rs_copy(b, k):
        return remote(rs_send.at[b, pl.ds(other(k) * PART, PART), :], rs_recv.at[b, k - 1], rs_ss.at[b, k - 1], rs_rs.at[b, k - 1], peers[k - 1])

    def ag_copy(b, k):
        rows = pl.ds(pl.multiple_of(b * QB + core * HALF + chip * PART, PART), PART)
        return remote(y_ref.at[rows, :], y_ref.at[rows, :], ag_ss.at[b, k - 1], ag_rs.at[b, k - 1], peers[k - 1])

    def fw_copy(b):
        rows = pl.ds(pl.multiple_of(b * QB + core * HALF, HALF), HALF)
        return remote(y_ref.at[rows, :], y_ref.at[rows, :], fw_ss.at[b], fw_rs.at[b], partner)

    def output(b):
        term = sum(dot(o_v[i], wo_v[pl.ds(i * 256, 256), :]) for i in range(PAIRS))
        acc_v[b % 2] = term
        pair_send[b] = acc_v[b % 2, pl.ds(theirs, HALF), :].astype(BF16)
        pair_copy(b).start()

    def chip_sum(b):
        pair_copy(b).wait_recv()
        total = acc_v[b % 2, pl.ds(mine, HALF), :] + pair_recv[b].astype(F32)
        acc_v[b % 2, pl.ds(mine, HALF), :] = total
        rs_send[b] = total.astype(BF16)
        own_v[b] = acc_v[b % 2, pl.ds(pl.multiple_of(core * HALF + chip * PART, PART), PART), :]
        for k in range(1, CHIPS):
            rs_copy(b, k).start()

    def finish(b):
        total = own_v[b]
        for k in range(1, CHIPS):
            rs_copy(b, k).wait_recv()
        for k in range(1, CHIPS):
            total = total + rs_recv[b, k - 1].astype(F32)
        rows = pl.ds(pl.multiple_of(b * QB + core * HALF + chip * PART, PART), PART)
        y_ref[rows, :] = (x_v[rows, :].astype(F32) + total).astype(BF16)
        for k in range(1, CHIPS):
            ag_copy(b, k).start()

    def forward(b):
        for k in range(1, CHIPS):
            ag_copy(b, k).wait_recv()
        fw_copy(b).start()

    for b in range(NB):
        if b % (PB // QB) == 0:
            project(b // (PB // QB))

        def hook(b=b):
            if b >= 1:
                chip_sum(b - 1)
            if b >= 2:
                forward(b - 2)

        attention(b, hook)
        if b >= 1:
            finish(b - 1)
        if b == 0:
            loads["wo"].wait()
            pl.semaphore_wait(barrier, CHIPS)
        output(b)
    chip_sum(NB - 1)
    forward(NB - 2)
    finish(NB - 1)
    forward(NB - 1)
    for b in range(NB):
        fw_copy(b).wait_recv()
        pair_copy(b).wait_send()
        for k in range(1, CHIPS):
            rs_copy(b, k).wait_send()
            ag_copy(b, k).wait_send()
        fw_copy(b).wait_send()


def solution(mesh):
    near, far = rotary_tables()

    def step(x, gain, wq, wk, wv, wo):
        vmem, anywhere = pl.BlockSpec(memory_space=pltpu.VMEM), pl.BlockSpec(memory_space=pl.ANY)
        dma = pltpu.SemaphoreType.DMA
        return pl.pallas_call(
            kernel,
            out_shape=jax.ShapeDtypeStruct((ROWS, D), BF16),
            in_specs=[anywhere, vmem, anywhere, vmem, anywhere, anywhere, anywhere, anywhere],
            out_specs=vmem,
            scratch_shapes=[
                pltpu.VMEM((ROWS, D), BF16),
                pltpu.VMEM((2, PB, HEAD), F32),
                pltpu.VMEM((PAIRS, D, 256), BF16),
                pltpu.VMEM((PAIRS, D, 256), BF16),
                pltpu.VMEM((PAIRS, D, 256), BF16),
                pltpu.VMEM((D, D), BF16),
                pltpu.VMEM((PB, D), BF16),
                pltpu.VMEM((PB, HEAD), F32),
                pltpu.VMEM((PB, HEAD), F32),
                pltpu.VMEM((HEADS, ROWS, HEAD), BF16),
                pltpu.VMEM((HEADS, ROWS, HEAD), BF16),
                pltpu.VMEM((HEADS, WIDE, ROWS), BF16),
                pltpu.VMEM((ROWS, QB), F32),
                pltpu.VMEM((ROWS, QB), F32),
                pltpu.VMEM((PAIRS, QB, 256), BF16),
                pltpu.VMEM((2, QB, D), F32),
                pltpu.VMEM((NB, HALF, D), BF16),
                pltpu.VMEM((NB, HALF, D), BF16),
                pltpu.VMEM((NB, HALF, D), BF16),
                pltpu.VMEM((NB, CHIPS - 1, PART, D), BF16),
                pltpu.VMEM((NB, PART, D), F32),
                dma((18,)), dma((NB,)), dma((NB,)), dma((NB, CHIPS - 1)), dma((NB, CHIPS - 1)), dma((NB, CHIPS - 1)), dma((NB, CHIPS - 1)),
                dma((NB,)), dma((NB,)),
            ],
            compiler_params=pltpu.CompilerParams(collective_id=0, has_side_effects=True, vmem_limit_bytes=60 * 2**20),
            cost_estimate=pl.CostEstimate(flops=26 * 10**9, transcendentals=20 * 10**6, bytes_accessed=20 * 2**20),
        )(x, gain.reshape(1, D), jnp.asarray(near), jnp.asarray(far), wq, wk, wv, wo)

    tokens, columns = P("dp", None), P(None, "tp")
    return jax.shard_map(
        step,
        mesh=mesh,
        in_specs=(tokens, P(None), columns, columns, columns, P("tp", None)),
        out_specs=tokens,
        check_vma=False,
    )
```

```python
import functools

import jax
import jax.numpy as jnp
import numpy as np
from jax import lax
from jax.experimental import pallas as pl
from jax.experimental.pallas import tpu as pltpu
from jax.sharding import PartitionSpec as P

HEAD = 128
THETA = 10000
LOG2E = 1.4426950408889634
ROWS, D = 2048, 1024
HEADS = 8
PAIRS = HEADS // 2
GROUP = 4
QB = 256
NB = ROWS // QB
PB = 512
KC = 256
WIDE = HEAD + 16
HALF = QB // 2
PART = HALF // 8
CHIPS = 8
SCALE = HEAD**-0.5
F32, BF16 = jnp.float32, jnp.bfloat16


def dot(a, b, ca=1, cb=0):
    return lax.dot_general(a, b, (((ca,), (cb,)), ((), ())), preferred_element_type=F32)


class Plan:
    def __init__(self):
        self.clock, self.wire, self.waiting = 5.0, 0.0, []

    def send(self, stage, b):
        if stage == 0:
            ready = self.clock + 2
        else:
            self.wire = max(self.wire, self.clock) + 2.9
            ready = self.wire + 4
        self.waiting.append((ready, stage, b))

    def due(self, rest=False):
        done = []
        while self.waiting:
            first = min(self.waiting)
            if first[0] > self.clock and not rest:
                break
            self.waiting.remove(first)
            self.clock = max(self.clock, first[0])
            done.append(first[1:])
            if first[1] < 2:
                self.send(first[1] + 1, first[2])
        return done


def rotary_tables():
    half = HEAD // 2
    rate = THETA ** (-np.arange(half) / half)

    def both(place):
        angle = place[:, None] * rate
        cos, sin = np.cos(angle), np.sin(angle)
        return np.concatenate([cos, cos], 1).astype(np.float32), np.concatenate([-sin, sin], 1).astype(np.float32)

    near = both(np.arange(PB, dtype=np.float64))
    far = both(np.arange(ROWS // PB, dtype=np.float64) * PB)
    far = tuple(np.concatenate([f, np.zeros((8 - f.shape[0], HEAD), np.float32)]) for f in far)
    return np.stack(near), np.stack(far)


def kernel(x_hbm, gain_ref, near_hbm, far_ref, wq_hbm, wk_hbm, wv_hbm, wo_hbm, y_ref,
           x_v, near_v, wq_v, wk_v, wv_v, wo_v, h_v, cos_v, sin_v, q_v, k_v, vt_v, s0_v, s1_v, o_v, acc_v,
           pair_send, pair_recv, rs_send, rs_recv, own_v,
           in_sem, pair_ss, pair_rs, rs_ss, rs_rs, ag_ss, ag_rs, fw_ss, fw_rs):
    dp, me = lax.axis_index("dp"), lax.axis_index("tp")
    core = lax.rem(me, 2)
    chip = lax.div(me, 2)
    bits = [lax.rem(lax.div(chip, 4), 2), lax.rem(lax.div(chip, 2), 2), lax.rem(chip, 2)]

    def other(k):
        at = [1 - b if (k >> (2 - i)) & 1 else b for i, b in enumerate(bits)]
        return at[0] * 4 + at[1] * 2 + at[2]

    def device(chip_, core_):
        return {"tp": chip_ * 2 + core_}

    partner = device(chip, 1 - core)
    peers = [device(other(k), core) for k in range(1, CHIPS)]

    def fetch(i, src, dst):
        return pltpu.make_async_copy(src, dst, in_sem.at[i])

    loads = {}
    for p in range(ROWS // PB):
        loads["x", p] = fetch(p, x_hbm.at[pl.ds(p * PB, PB), :], x_v.at[pl.ds(p * PB, PB), :])
    loads["near"] = fetch(4, near_hbm, near_v)
    for c in range(PAIRS):
        for n, (name, src, dst) in enumerate((("q", wq_hbm, wq_v), ("k", wk_hbm, wk_v), ("v", wv_hbm, wv_v))):
            loads[name, c] = fetch(5 + 3 * c + n, src.at[:, pl.ds(c * 256, 256)], dst.at[c])
    loads["wo"] = fetch(17, wo_hbm, wo_v)
    order = [("x", 0), "near"] + [(n, c) for c in range(PAIRS) for n in "qkv"] + [("x", 1), "wo", ("x", 2), ("x", 3)]
    for key in order:
        loads[key].start()

    barrier = pltpu.get_barrier_semaphore()
    for peer in [partner] + peers:
        pl.semaphore_signal(barrier, inc=1, device_id=peer, device_id_type=pl.DeviceIdType.MESH)

    for h in range(HEADS):
        vt_v[h, HEAD:, :] = jnp.ones((WIDE - HEAD, ROWS), BF16)

    def normed(p):
        rows = pl.ds(p * PB, PB)
        loads["x", p].wait()
        wide = x_v[rows, :].astype(F32)
        scale = lax.rsqrt(jnp.mean(wide * wide, -1, keepdims=True) + 1e-6)
        h_v[...] = (wide * scale * gain_ref[...].reshape(1, D).astype(F32)).astype(BF16)
        if p == 0:
            loads["near"].wait()
            cos_v[...] = near_v[0]
            sin_v[...] = near_v[1]
        else:
            cf, sf = far_ref[0, p : p + 1, :], far_ref[1, p : p + 1, :]
            cn, sn = near_v[0], near_v[1]
            cos_v[...] = cn * cf - sn * sf
            sin_v[...] = sn * cf + cn * sf

    def project(p, hook):
        rows = pl.ds(p * PB, PB)

        def turned(t):
            t = t.astype(BF16).astype(F32)
            return (t * cos_v[...] + pltpu.roll(t, HEAD // 2, 1) * sin_v[...]).astype(BF16)

        def body(c, _):
            @pl.when(c == 2)
            def _():
                hook()

            if p == 0:
                for n, (src, dst) in enumerate(((wq_hbm, wq_v), (wk_hbm, wk_v), (wv_hbm, wv_v))):
                    pltpu.make_async_copy(src.at[:, pl.ds(0, 256)], dst.at[c], in_sem.at[5 + 3 * c + n]).wait()
            a = h_v[...]
            tq = dot(a, wq_v[c])
            tk = dot(a, wk_v[c])
            tv = dot(a, wv_v[c])
            for n in range(2):
                lanes = slice(n * HEAD, (n + 1) * HEAD)
                q_v[2 * c + n, rows, :] = turned(tq[:, lanes])
                k_v[2 * c + n, rows, :] = turned(tk[:, lanes])
                vt_v[2 * c + n, :HEAD, rows] = tv[:, lanes].astype(BF16).T
            return 0

        lax.fori_loop(0, PAIRS, body, 0)

    e = SCALE * LOG2E

    def attention(b, hook):
        rows = pl.ds(b * QB, QB)
        n = b + 1

        def score(h, c, s_v, top):
            s = dot(k_v[h, pl.ds(c * KC, KC), :], q_v[h, rows, :], 1, 1)
            if c == b:
                ok = lax.broadcasted_iota(jnp.int32, (KC, QB), 0) <= lax.broadcasted_iota(jnp.int32, (KC, QB), 1)
                s = jnp.where(ok, s, -jnp.inf)
            s_v[pl.ds(c * KC, KC), :] = s
            m = s.reshape(KC // 8, 8, QB).max(axis=0)
            return m if top is None else jnp.maximum(top, m)

        def mixed(h, c, s_v, top, acc):
            w = jnp.exp2((s_v[pl.ds(c * KC, KC), :] - top) * e).astype(BF16)
            m = dot(vt_v[h, :, pl.ds(c * KC, KC)], w)
            return m if acc is None else acc + m

        def step(h, s_v, top, h_next, s_next):
            acc = new = None
            top = top.max(axis=0, keepdims=True)
            for c in range(n):
                if h_next is not None:
                    new = score(h_next, c, s_next, new)
                acc = mixed(h, c, s_v, top, acc)
            out = acc[:HEAD, :] * (1 / acc[HEAD : HEAD + 1, :])
            return out.T.astype(BF16), new

        def body(i, _):
            @pl.when(i == 1)
            def _():
                hook()

            top = None
            for c in range(n):
                top = score(GROUP * i, c, s0_v, top)
            for j in range(GROUP):
                h = GROUP * i + j
                now, later = (s0_v, s1_v) if j % 2 == 0 else (s1_v, s0_v)
                out, top = step(h, now, top, h + 1 if j < GROUP - 1 else None, later)
                o_v[GROUP // 2 * i + j // 2, :, (j % 2) * HEAD : (j % 2 + 1) * HEAD] = out
            return 0

        lax.fori_loop(0, HEADS // GROUP, body, 0)

    def remote(src, dst, ss, rs, dev):
        return pltpu.make_async_remote_copy(src_ref=src, dst_ref=dst, send_sem=ss, recv_sem=rs, device_id=dev,
                                            device_id_type=pl.DeviceIdType.MESH)

    mine = pl.multiple_of(core * HALF, HALF)
    theirs = pl.multiple_of((1 - core) * HALF, HALF)

    def pair_copy(b):
        return remote(pair_send.at[b], pair_recv.at[b], pair_ss.at[b], pair_rs.at[b], partner)

    def rs_copy(b, k):
        return remote(rs_send.at[b, pl.ds(other(k) * PART, PART), :], rs_recv.at[b, k - 1], rs_ss.at[b, k - 1], rs_rs.at[b, k - 1], peers[k - 1])

    def ag_copy(b, k):
        rows = pl.ds(pl.multiple_of(b * QB + core * HALF + chip * PART, PART), PART)
        return remote(y_ref.at[rows, :], y_ref.at[rows, :], ag_ss.at[b, k - 1], ag_rs.at[b, k - 1], peers[k - 1])

    def fw_copy(b):
        rows = pl.ds(pl.multiple_of(b * QB + core * HALF, HALF), HALF)
        return remote(y_ref.at[rows, :], y_ref.at[rows, :], fw_ss.at[b], fw_rs.at[b], partner)

    def output(b):
        term = sum(dot(o_v[i], wo_v[pl.ds(i * 256, 256), :]) for i in range(PAIRS))
        if b % 2 == 1 and b < NB - 1:
            normed((b + 1) // 2)
        acc_v[b % 2] = term
        pair_send[b] = acc_v[b % 2, pl.ds(theirs, HALF), :].astype(BF16)
        pair_copy(b).start()

    def chip_sum(b):
        pair_copy(b).wait_recv()
        rs_send[b] = (acc_v[b % 2, pl.ds(mine, HALF), :] + pair_recv[b].astype(F32)).astype(BF16)
        for k in range(1, CHIPS):
            rs_copy(b, k).start()
        part = pl.multiple_of(chip * PART, PART)
        own_v[b] = acc_v[b % 2, pl.ds(mine + part, PART), :] + pair_recv[b, pl.ds(part, PART), :].astype(F32)

    def finish(b):
        total = own_v[b]
        for k in range(1, CHIPS):
            rs_copy(b, k).wait_recv()
        for k in range(1, CHIPS):
            total = total + rs_recv[b, k - 1].astype(F32)
        rows = pl.ds(pl.multiple_of(b * QB + core * HALF + chip * PART, PART), PART)
        y_ref[rows, :] = (x_v[rows, :].astype(F32) + total).astype(BF16)
        for k in range(1, CHIPS):
            ag_copy(b, k).start()

    def forward(b):
        for k in range(1, CHIPS):
            ag_copy(b, k).wait_recv()
        fw_copy(b).start()

    plan = Plan()

    def stages(due):
        for stage, b in due:
            (chip_sum, finish, forward)[stage](b)

    normed(0)
    for b in range(NB):
        if b % 2 == 0:
            stages(plan.due())
            plan.clock += 1.9
            middle = plan.due()
            project(b // 2, lambda: stages(middle))
            plan.clock += 1.9
        stages(plan.due())
        plan.clock += 0.9 + 0.27 * b
        middle = plan.due()
        attention(b, lambda: stages(middle))
        plan.clock += 0.9 + 0.27 * b
        stages(plan.due())
        if b == 0:
            loads["wo"].wait()
            pl.semaphore_wait(barrier, CHIPS)
        output(b)
        plan.clock += 0.8
        plan.send(0, b)
    stages(plan.due(rest=True))
    for b in range(NB):
        fw_copy(b).wait_recv()
        pair_copy(b).wait_send()
        for k in range(1, CHIPS):
            rs_copy(b, k).wait_send()
            ag_copy(b, k).wait_send()
        fw_copy(b).wait_send()


def solution(mesh):
    near, far = rotary_tables()

    def step(x, gain, wq, wk, wv, wo):
        vmem, anywhere = pl.BlockSpec(memory_space=pltpu.VMEM), pl.BlockSpec(memory_space=pltpu.HBM)
        dma = pltpu.SemaphoreType.DMA
        return pl.pallas_call(
            kernel,
            out_shape=pltpu.VMEM((ROWS, D), BF16),
            in_specs=[anywhere, vmem, anywhere, vmem, anywhere, anywhere, anywhere, anywhere],
            out_specs=vmem,
            scratch_shapes=[
                pltpu.VMEM((ROWS, D), BF16),
                pltpu.VMEM((2, PB, HEAD), F32),
                pltpu.VMEM((PAIRS, D, 256), BF16),
                pltpu.VMEM((PAIRS, D, 256), BF16),
                pltpu.VMEM((PAIRS, D, 256), BF16),
                pltpu.VMEM((D, D), BF16),
                pltpu.VMEM((PB, D), BF16),
                pltpu.VMEM((PB, HEAD), F32),
                pltpu.VMEM((PB, HEAD), F32),
                pltpu.VMEM((HEADS, ROWS, HEAD), BF16),
                pltpu.VMEM((HEADS, ROWS, HEAD), BF16),
                pltpu.VMEM((HEADS, WIDE, ROWS), BF16),
                pltpu.VMEM((ROWS, QB), F32),
                pltpu.VMEM((ROWS, QB), F32),
                pltpu.VMEM((PAIRS, QB, 256), BF16),
                pltpu.VMEM((2, QB, D), F32),
                pltpu.VMEM((NB, HALF, D), BF16),
                pltpu.VMEM((NB, HALF, D), BF16),
                pltpu.VMEM((NB, HALF, D), BF16),
                pltpu.VMEM((NB, CHIPS - 1, PART, D), BF16),
                pltpu.VMEM((NB, PART, D), F32),
                dma((18,)), dma((NB,)), dma((NB,)), dma((NB, CHIPS - 1)), dma((NB, CHIPS - 1)), dma((NB, CHIPS - 1)), dma((NB, CHIPS - 1)),
                dma((NB,)), dma((NB,)),
            ],
            compiler_params=pltpu.CompilerParams(collective_id=0, has_side_effects=True, vmem_limit_bytes=56 * 2**20),
            cost_estimate=pl.CostEstimate(flops=26 * 10**9, transcendentals=20 * 10**6, bytes_accessed=20 * 2**20),
        )(x, gain, jnp.asarray(near), jnp.asarray(far), wq, wk, wv, wo)

    tokens, columns = P("dp", None), P(None, "tp")
    return jax.shard_map(
        step,
        mesh=mesh,
        in_specs=(tokens, P(None), columns, columns, columns, P("tp", None)),
        out_specs=tokens,
        check_vma=False,
    )
```

```python
import functools

import jax
import jax.numpy as jnp
import numpy as np
from jax import lax
from jax.experimental import pallas as pl
from jax.experimental.pallas import tpu as pltpu
from jax.sharding import PartitionSpec as P

HEAD = 128
THETA = 10000
LOG2E = 1.4426950408889634
ROWS, D = 2048, 1024
HEADS = 8
PAIRS = HEADS // 2
GROUP = 4
QB = 256
NB = ROWS // QB
PB = 512
KC = 256
WIDE = HEAD + 16
HALF = QB // 2
PART = HALF // 8
CHIPS = 8
SCALE = HEAD**-0.5
F32, BF16 = jnp.float32, jnp.bfloat16


def dot(a, b, ca=1, cb=0):
    return lax.dot_general(a, b, (((ca,), (cb,)), ((), ())), preferred_element_type=F32)


FAR_FIRST = (7, 6, 5, 3, 4, 2, 1)
ATTENTION = (1.1, 1.6, 2.3, 2.7, 3.4, 4.1, 4.6, 5.2)
SPLIT = 2


def parts(b):
    return SPLIT if b == NB - 1 else 1


class Plan:
    def __init__(self):
        self.clock, self.wire, self.waiting = 4.5, 0.0, []

    def send(self, stage, b, s, later=0):
        if stage == 0:
            ready = self.clock + 2 + later
        else:
            self.wire = max(self.wire, self.clock) + 3 / parts(b)
            ready = self.wire + 3.8
        self.waiting.append((ready, stage, b, s))

    def due(self, rest=False):
        done = []
        while self.waiting:
            first = min(self.waiting)
            if first[0] > self.clock and not rest:
                break
            self.waiting.remove(first)
            self.clock = max(self.clock, first[0])
            done.append(first[1:])
            if first[1] < 2:
                self.send(first[1] + 1, *first[2:])
        return done


def rotary_tables():
    half = HEAD // 2
    rate = THETA ** (-np.arange(half) / half)

    def both(place):
        angle = place[:, None] * rate
        cos, sin = np.cos(angle), np.sin(angle)
        return np.concatenate([cos, cos], 1).astype(np.float32), np.concatenate([-sin, sin], 1).astype(np.float32)

    near = both(np.arange(PB, dtype=np.float64))
    far = both(np.arange(ROWS // PB, dtype=np.float64) * PB)
    far = tuple(np.concatenate([f, np.zeros((8 - f.shape[0], HEAD), np.float32)]) for f in far)
    return np.stack(near), np.stack(far)


def kernel(x_hbm, gain_ref, near_hbm, far_ref, wq_hbm, wk_hbm, wv_hbm, wo_hbm, y_ref,
           x_v, near_v, wq_v, wk_v, wv_v, wo_v, h_v, cos_v, sin_v, q_v, k_v, vt_v, s0_v, s1_v, o_v, acc_v,
           pair_send, pair_recv, rs_send, rs_recv, own_v,
           in_sem, pair_ss, pair_rs, rs_ss, rs_rs, ag_ss, ag_rs, fw_ss, fw_rs):
    dp, me = lax.axis_index("dp"), lax.axis_index("tp")
    core = lax.rem(me, 2)
    chip = lax.div(me, 2)
    bits = [lax.rem(lax.div(chip, 4), 2), lax.rem(lax.div(chip, 2), 2), lax.rem(chip, 2)]

    def other(k):
        at = [1 - b if (k >> (2 - i)) & 1 else b for i, b in enumerate(bits)]
        return at[0] * 4 + at[1] * 2 + at[2]

    def device(chip_, core_):
        return {"tp": chip_ * 2 + core_}

    partner = device(chip, 1 - core)
    peers = [device(other(k), core) for k in range(1, CHIPS)]

    def fetch(i, src, dst):
        return pltpu.make_async_copy(src, dst, in_sem.at[i])

    loads = {}
    for p in range(ROWS // PB):
        loads["x", p] = fetch(p, x_hbm.at[pl.ds(p * PB, PB), :], x_v.at[pl.ds(p * PB, PB), :])
    loads["near"] = fetch(4, near_hbm, near_v)
    for c in range(PAIRS):
        for n, (name, src, dst) in enumerate((("q", wq_hbm, wq_v), ("k", wk_hbm, wk_v), ("v", wv_hbm, wv_v))):
            loads[name, c] = fetch(5 + 3 * c + n, src.at[:, pl.ds(c * 256, 256)], dst.at[c])
    loads["wo"] = fetch(17, wo_hbm, wo_v)
    order = [("x", 0), "near"] + [(n, c) for c in range(PAIRS) for n in "qkv"] + [("x", 1), "wo", ("x", 2), ("x", 3)]
    early = 5
    for key in order[:early]:
        loads[key].start()

    barrier = pltpu.get_barrier_semaphore()
    for peer in [partner] + peers:
        pl.semaphore_signal(barrier, inc=1, device_id=peer, device_id_type=pl.DeviceIdType.MESH)

    for h in range(HEADS):
        vt_v[h, HEAD:, :] = jnp.ones((WIDE - HEAD, ROWS), BF16)

    def normed(p):
        rows = pl.ds(p * PB, PB)
        loads["x", p].wait()
        if p == 0:
            for key in order[early:]:
                loads[key].start()
        wide = x_v[rows, :].astype(F32)
        scale = lax.rsqrt(jnp.mean(wide * wide, -1, keepdims=True) + 1e-6)
        h_v[...] = (wide * scale * gain_ref[...].reshape(1, D).astype(F32)).astype(BF16)
        if p == 0:
            loads["near"].wait()
            cos_v[...] = near_v[0]
            sin_v[...] = near_v[1]
        else:
            cf, sf = far_ref[0, p : p + 1, :], far_ref[1, p : p + 1, :]
            cn, sn = near_v[0], near_v[1]
            cos_v[...] = cn * cf - sn * sf
            sin_v[...] = sn * cf + cn * sf

    def project(p, hooks):
        rows = pl.ds(p * PB, PB)

        def turned(t):
            t = t.astype(BF16).astype(F32)
            return (t * cos_v[...] + pltpu.roll(t, HEAD // 2, 1) * sin_v[...]).astype(BF16)

        def body(c, _):
            for at, due in hooks.items():

                @pl.when(c == at)
                def _(due=due):
                    stages(due)

            if p == 0:
                for n, (src, dst) in enumerate(((wq_hbm, wq_v), (wk_hbm, wk_v), (wv_hbm, wv_v))):
                    pltpu.make_async_copy(src.at[:, pl.ds(0, 256)], dst.at[c], in_sem.at[5 + 3 * c + n]).wait()
            a = h_v[...]
            tq = dot(a, wq_v[c])
            tk = dot(a, wk_v[c])
            tv = dot(a, wv_v[c])
            for n in range(2):
                lanes = slice(n * HEAD, (n + 1) * HEAD)
                q_v[2 * c + n, rows, :] = turned(tq[:, lanes])
                k_v[2 * c + n, rows, :] = turned(tk[:, lanes])
                vt_v[2 * c + n, :HEAD, rows] = tv[:, lanes].astype(BF16).T
            return 0

        lax.fori_loop(0, PAIRS, body, 0)

    e = SCALE * LOG2E

    def attention(b, hook):
        rows = pl.ds(b * QB, QB)
        n = b + 1

        def score(h, c, s_v, top):
            s = dot(k_v[h, pl.ds(c * KC, KC), :], q_v[h, rows, :], 1, 1)
            if c == b:
                ok = lax.broadcasted_iota(jnp.int32, (KC, QB), 0) <= lax.broadcasted_iota(jnp.int32, (KC, QB), 1)
                s = jnp.where(ok, s, -jnp.inf)
            s_v[pl.ds(c * KC, KC), :] = s
            m = s.reshape(KC // 8, 8, QB).max(axis=0)
            return m if top is None else jnp.maximum(top, m)

        def score2(h, c, s_v, top):
            two = min(2, n - c)
            s = dot(k_v[h, pl.ds(c * KC, two * KC), :], q_v[h, rows, :], 1, 1)
            if c + two - 1 == b:
                ok = lax.broadcasted_iota(jnp.int32, (two * KC, QB), 0) <= lax.broadcasted_iota(jnp.int32, (two * KC, QB), 1) + (two - 1) * KC
                s = jnp.where(ok, s, -jnp.inf)
            s_v[pl.ds(c * KC, two * KC), :] = s
            m = s.reshape(two * KC // 8, 8, QB).max(axis=0)
            return m if top is None else jnp.maximum(top, m)

        def mixed(h, c, s_v, top, acc):
            w = jnp.exp2((s_v[pl.ds(c * KC, KC), :] - top) * e).astype(BF16)
            m = dot(vt_v[h, :, pl.ds(c * KC, KC)], w)
            return m if acc is None else acc + m

        def step(h, s_v, top, h_next, s_next):
            acc = new = None
            top = top.max(axis=0, keepdims=True)
            for c in range(n):
                if h_next is not None and c % 2 == 0:
                    new = score2(h_next, c, s_next, new)
                acc = mixed(h, c, s_v, top, acc)
            out = acc[:HEAD, :] * (1 / acc[HEAD : HEAD + 1, :])
            return out.T.astype(BF16), new

        def body(i, _):
            @pl.when(i == 1)
            def _():
                hook()

            top = None
            for c in range(0, n, 2):
                top = score2(GROUP * i, c, s0_v, top)
            for j in range(GROUP):
                h = GROUP * i + j
                now, later = (s0_v, s1_v) if j % 2 == 0 else (s1_v, s0_v)
                out, top = step(h, now, top, h + 1 if j < GROUP - 1 else None, later)
                o_v[GROUP // 2 * i + j // 2, :, (j % 2) * HEAD : (j % 2 + 1) * HEAD] = out
            return 0

        lax.fori_loop(0, HEADS // GROUP, body, 0)

    def remote(src, dst, ss, rs, dev):
        return pltpu.make_async_remote_copy(src_ref=src, dst_ref=dst, send_sem=ss, recv_sem=rs, device_id=dev,
                                            device_id_type=pl.DeviceIdType.MESH)

    mine = pl.multiple_of(core * HALF, HALF)
    theirs = pl.multiple_of((1 - core) * HALF, HALF)

    def columns(b, s):
        width = D // parts(b)
        return pl.ds(s * width, width)

    def pair_copy(b, s):
        cols = columns(b, s)
        return remote(pair_send.at[b, :, cols], pair_recv.at[b, :, cols], pair_ss.at[b, s], pair_rs.at[b, s], partner)

    def rs_copy(b, s, k):
        cols = columns(b, s)
        return remote(rs_send.at[b, pl.ds(other(k) * PART, PART), cols], rs_recv.at[b, k - 1, :, cols],
                      rs_ss.at[b, s, k - 1], rs_rs.at[b, s, k - 1], peers[k - 1])

    def ag_copy(b, s, k):
        here = y_ref.at[pl.ds(pl.multiple_of(b * QB + core * HALF + chip * PART, PART), PART), columns(b, s)]
        return remote(here, here, ag_ss.at[b, s, k - 1], ag_rs.at[b, s, k - 1], peers[k - 1])

    def fw_copy(b, s):
        here = y_ref.at[pl.ds(pl.multiple_of(b * QB + core * HALF, HALF), HALF), columns(b, s)]
        return remote(here, here, fw_ss.at[b, s], fw_rs.at[b, s], partner)

    def term(b, rows):
        return sum(dot(o_v[i, rows, :], wo_v[pl.ds(i * 256, 256), :]) for i in range(PAIRS))

    def output(b):
        if b < NB - 1:
            whole = term(b, slice(None))
            if b % 2 == 1:
                normed((b + 1) // 2)
            acc_v[b % 2] = whole
            pair_send[b] = acc_v[b % 2, pl.ds(theirs, HALF), :].astype(BF16)
            pair_copy(b, 0).start()
        else:
            pair_send[b] = term(b, pl.ds(theirs, HALF)).astype(BF16)
            for s in range(parts(b)):
                pair_copy(b, s).start()
            acc_v[b % 2, pl.ds(mine, HALF), :] = term(b, pl.ds(mine, HALF))

    def chip_sum(b, s):
        cols = columns(b, s)
        pair_copy(b, s).wait_recv()
        rs_send[b, :, cols] = (acc_v[b % 2, pl.ds(mine, HALF), cols] + pair_recv[b, :, cols].astype(F32)).astype(BF16)
        for k in FAR_FIRST:
            rs_copy(b, s, k).start()
        part = pl.multiple_of(chip * PART, PART)
        own_v[b, :, cols] = acc_v[b % 2, pl.ds(mine + part, PART), cols] + pair_recv[b, pl.ds(part, PART), cols].astype(F32)

    def finish(b, s):
        cols = columns(b, s)
        total = own_v[b, :, cols]
        for k in range(1, CHIPS):
            rs_copy(b, s, k).wait_recv()
        for k in range(1, CHIPS):
            total = total + rs_recv[b, k - 1, :, cols].astype(F32)
        rows = pl.ds(pl.multiple_of(b * QB + core * HALF + chip * PART, PART), PART)
        y_ref[rows, cols] = (x_v[rows, cols].astype(F32) + total).astype(BF16)
        for k in FAR_FIRST:
            ag_copy(b, s, k).start()

    def forward(b, s):
        for k in range(1, CHIPS):
            ag_copy(b, s, k).wait_recv()
        fw_copy(b, s).start()

    plan = Plan()

    def stages(due):
        for stage, b, s in due:
            (chip_sum, finish, forward)[stage](b, s)

    normed(0)
    for b in range(NB):
        if b % 2 == 0:
            stages(plan.due())
            hooks = {}
            for c in range(1, PAIRS):
                plan.clock += 0.95
                if due := plan.due():
                    hooks[c] = due
            project(b // 2, hooks)
            plan.clock += 0.95
        stages(plan.due())
        plan.clock += ATTENTION[b] / 2
        middle = plan.due()
        attention(b, lambda: stages(middle))
        plan.clock += ATTENTION[b] / 2
        stages(plan.due())
        if b == 0:
            loads["wo"].wait()
            pl.semaphore_wait(barrier, CHIPS)
        output(b)
        plan.clock += 0.8
        plan.send(0, b, 0, -0.4 if b == NB - 1 else 0)
        for s in range(1, parts(b)):
            plan.send(0, b, s, 0.2)
    stages(plan.due(rest=True))
    for b in range(NB):
        for s in range(parts(b)):
            fw_copy(b, s).wait_recv()
            pair_copy(b, s).wait_send()
            for k in range(1, CHIPS):
                rs_copy(b, s, k).wait_send()
                ag_copy(b, s, k).wait_send()
            fw_copy(b, s).wait_send()


def solution(mesh):
    near, far = rotary_tables()

    def step(x, gain, wq, wk, wv, wo):
        vmem, anywhere = pl.BlockSpec(memory_space=pltpu.VMEM), pl.BlockSpec(memory_space=pltpu.HBM)
        dma = pltpu.SemaphoreType.DMA
        return pl.pallas_call(
            kernel,
            out_shape=pltpu.VMEM((ROWS, D), BF16),
            in_specs=[anywhere, vmem, anywhere, vmem, anywhere, anywhere, anywhere, anywhere],
            out_specs=vmem,
            scratch_shapes=[
                pltpu.VMEM((ROWS, D), BF16),
                pltpu.VMEM((2, PB, HEAD), F32),
                pltpu.VMEM((PAIRS, D, 256), BF16),
                pltpu.VMEM((PAIRS, D, 256), BF16),
                pltpu.VMEM((PAIRS, D, 256), BF16),
                pltpu.VMEM((D, D), BF16),
                pltpu.VMEM((PB, D), BF16),
                pltpu.VMEM((PB, HEAD), F32),
                pltpu.VMEM((PB, HEAD), F32),
                pltpu.VMEM((HEADS, ROWS, HEAD), BF16),
                pltpu.VMEM((HEADS, ROWS, HEAD), BF16),
                pltpu.VMEM((HEADS, WIDE, ROWS), BF16),
                pltpu.VMEM((ROWS, QB), F32),
                pltpu.VMEM((ROWS, QB), F32),
                pltpu.VMEM((PAIRS, QB, 256), BF16),
                pltpu.VMEM((2, QB, D), F32),
                pltpu.VMEM((NB, HALF, D), BF16),
                pltpu.VMEM((NB, HALF, D), BF16),
                pltpu.VMEM((NB, HALF, D), BF16),
                pltpu.VMEM((NB, CHIPS - 1, PART, D), BF16),
                pltpu.VMEM((NB, PART, D), F32),
                dma((18,)), dma((NB, SPLIT)), dma((NB, SPLIT)), *[dma((NB, SPLIT, CHIPS - 1))] * 4, dma((NB, SPLIT)), dma((NB, SPLIT)),
            ],
            compiler_params=pltpu.CompilerParams(collective_id=0, has_side_effects=True, vmem_limit_bytes=56 * 2**20),
            cost_estimate=pl.CostEstimate(flops=26 * 10**9, transcendentals=20 * 10**6, bytes_accessed=20 * 2**20),
        )(x, gain, jnp.asarray(near), jnp.asarray(far), wq, wk, wv, wo)

    tokens, columns = P("dp", None), P(None, "tp")
    return jax.shard_map(
        step,
        mesh=mesh,
        in_specs=(tokens, P(None), columns, columns, columns, P("tp", None)),
        out_specs=tokens,
        check_vma=False,
    )
```

```python
import functools

import jax
import jax.numpy as jnp
import numpy as np
from jax import lax
from jax.experimental import pallas as pl
from jax.experimental.pallas import tpu as pltpu
from jax.sharding import PartitionSpec as P

HEAD = 128
THETA = 10000
LOG2E = 1.4426950408889634
ROWS, D = 2048, 1024
HEADS = 8
PAIRS = HEADS // 2
GROUP = 2
QB = 256
NB = ROWS // QB
PB = 512
KC = 256
WIDE = HEAD + 16
HALF = QB // 2
PART = HALF // 8
CHIPS = 8
SCALE = HEAD**-0.5
F32, BF16 = jnp.float32, jnp.bfloat16


def dot(a, b, ca=1, cb=0):
    return lax.dot_general(a, b, (((ca,), (cb,)), ((), ())), preferred_element_type=F32)


FAR_FIRST = (7, 6, 5, 3, 4, 2, 1)
ATTENTION = (1.1, 1.6, 2.3, 2.7, 3.4, 4.1, 4.6, 5.2)
SPLIT = 2


def parts(b):
    return SPLIT if b == NB - 1 else 1


class Plan:
    def __init__(self):
        self.clock, self.wire, self.waiting = 4.5, 0.0, []

    def send(self, stage, b, s, later=0):
        if stage == 0:
            ready = self.clock + 2 + later
        else:
            self.wire = max(self.wire, self.clock) + 3 / parts(b)
            ready = self.wire + 3.8
        self.waiting.append((ready, stage, b, s))

    def due(self, rest=False):
        done = []
        while self.waiting:
            first = min(self.waiting)
            if first[0] > self.clock and not rest:
                break
            self.waiting.remove(first)
            self.clock = max(self.clock, first[0])
            done.append(first[1:])
            if first[1] < 2:
                self.send(first[1] + 1, *first[2:])
        return done


def rotary_tables():
    half = HEAD // 2
    rate = THETA ** (-np.arange(half) / half)

    def both(place):
        angle = place[:, None] * rate
        cos, sin = np.cos(angle), np.sin(angle)
        return np.concatenate([cos, cos], 1).astype(np.float32), np.concatenate([-sin, sin], 1).astype(np.float32)

    near = both(np.arange(PB, dtype=np.float64))
    far = both(np.arange(ROWS // PB, dtype=np.float64) * PB)
    far = tuple(np.concatenate([f, np.zeros((8 - f.shape[0], HEAD), np.float32)]) for f in far)
    return np.stack(near), np.stack(far)


def kernel(x_hbm, gain_ref, near_hbm, far_ref, wq_hbm, wk_hbm, wv_hbm, wo_hbm, y_ref,
           x_v, near_v, wq_v, wk_v, wv_v, wo_v, h_v, cos_v, sin_v, q_v, k_v, vt_v, s0_v, s1_v, o_v, acc_v,
           pair_send, pair_recv, rs_send, rs_recv, own_v,
           in_sem, pair_ss, pair_rs, rs_ss, rs_rs, ag_ss, ag_rs, fw_ss, fw_rs):
    dp, me = lax.axis_index("dp"), lax.axis_index("tp")
    core = lax.rem(me, 2)
    chip = lax.div(me, 2)
    bits = [lax.rem(lax.div(chip, 4), 2), lax.rem(lax.div(chip, 2), 2), lax.rem(chip, 2)]

    def other(k):
        at = [1 - b if (k >> (2 - i)) & 1 else b for i, b in enumerate(bits)]
        return at[0] * 4 + at[1] * 2 + at[2]

    def device(chip_, core_):
        return {"tp": chip_ * 2 + core_}

    partner = device(chip, 1 - core)
    peers = [device(other(k), core) for k in range(1, CHIPS)]

    def fetch(i, src, dst):
        return pltpu.make_async_copy(src, dst, in_sem.at[i])

    loads = {}
    for p in range(ROWS // PB):
        loads["x", p] = fetch(p, x_hbm.at[pl.ds(p * PB, PB), :], x_v.at[pl.ds(p * PB, PB), :])
    loads["near"] = fetch(4, near_hbm, near_v)
    for c in range(PAIRS):
        for n, (name, src, dst) in enumerate((("q", wq_hbm, wq_v), ("k", wk_hbm, wk_v), ("v", wv_hbm, wv_v))):
            loads[name, c] = fetch(5 + 3 * c + n, src.at[:, pl.ds(c * 256, 256)], dst.at[c])
    loads["wo"] = fetch(17, wo_hbm, wo_v)
    order = [("x", 0), "near"] + [(n, c) for c in range(PAIRS) for n in "qkv"] + [("x", 1), "wo", ("x", 2), ("x", 3)]
    for key in order:
        loads[key].start()

    barrier = pltpu.get_barrier_semaphore()
    for peer in [partner] + peers:
        pl.semaphore_signal(barrier, inc=1, device_id=peer, device_id_type=pl.DeviceIdType.MESH)

    for h in range(HEADS):
        vt_v[h, HEAD:, :] = jnp.ones((WIDE - HEAD, ROWS), BF16)

    def normed(p):
        rows = pl.ds(p * PB, PB)
        loads["x", p].wait()
        wide = x_v[rows, :].astype(F32)
        scale = lax.rsqrt(jnp.mean(wide * wide, -1, keepdims=True) + 1e-6)
        h_v[...] = (wide * scale * gain_ref[...].reshape(1, D).astype(F32)).astype(BF16)
        if p == 0:
            loads["near"].wait()
            cos_v[...] = near_v[0]
            sin_v[...] = near_v[1]
        else:
            cf, sf = far_ref[0, p : p + 1, :], far_ref[1, p : p + 1, :]
            cn, sn = near_v[0], near_v[1]
            cos_v[...] = cn * cf - sn * sf
            sin_v[...] = sn * cf + cn * sf

    def project(p, hooks):
        rows = pl.ds(p * PB, PB)

        def turned(t):
            t = t.astype(BF16).astype(F32)
            return (t * cos_v[...] + pltpu.roll(t, HEAD // 2, 1) * sin_v[...]).astype(BF16)

        def body(c, _):
            for at, due in hooks.items():

                @pl.when(c == at)
                def _(due=due):
                    stages(due)

            if p == 0:
                for n, (src, dst) in enumerate(((wq_hbm, wq_v), (wk_hbm, wk_v), (wv_hbm, wv_v))):
                    pltpu.make_async_copy(src.at[:, pl.ds(0, 256)], dst.at[c], in_sem.at[5 + 3 * c + n]).wait()
            a = h_v[...]
            tq = dot(a, wq_v[c])
            tk = dot(a, wk_v[c])
            tv = dot(a, wv_v[c])
            for n in range(2):
                lanes = slice(n * HEAD, (n + 1) * HEAD)
                q_v[2 * c + n, rows, :] = turned(tq[:, lanes])
                k_v[2 * c + n, rows, :] = turned(tk[:, lanes])
                vt_v[2 * c + n, :HEAD, rows] = tv[:, lanes].astype(BF16).T
            return 0

        lax.fori_loop(0, PAIRS, body, 0)

    e = SCALE * LOG2E

    def attention(b, hooks):
        rows = pl.ds(b * QB, QB)
        n = b + 1

        def score(h, c, s_v, top):
            s = dot(k_v[h, pl.ds(c * KC, KC), :], q_v[h, rows, :], 1, 1)
            if c == b:
                ok = lax.broadcasted_iota(jnp.int32, (KC, QB), 0) <= lax.broadcasted_iota(jnp.int32, (KC, QB), 1)
                s = jnp.where(ok, s, -jnp.inf)
            s_v[pl.ds(c * KC, KC), :] = s
            m = s.reshape(KC // 8, 8, QB).max(axis=0)
            return m if top is None else jnp.maximum(top, m)

        def mixed(h, c, s_v, top, acc):
            w = jnp.exp2((s_v[pl.ds(c * KC, KC), :] - top) * e).astype(BF16)
            m = dot(vt_v[h, :, pl.ds(c * KC, KC)], w)
            return m if acc is None else acc + m

        def step(h, s_v, top, h_next, s_next):
            acc = new = None
            top = top.max(axis=0, keepdims=True)
            for c in range(n):
                if h_next is not None:
                    new = score(h_next, c, s_next, new)
                acc = mixed(h, c, s_v, top, acc)
            out = acc[:HEAD, :] * (1 / acc[HEAD : HEAD + 1, :])
            return out.T.astype(BF16), new

        def body(i, _):
            for at, due in hooks.items():

                @pl.when(i == at)
                def _(due=due):
                    stages(due)

            top = None
            for c in range(n):
                top = score(GROUP * i, c, s0_v, top)
            for j in range(GROUP):
                h = GROUP * i + j
                now, later = (s0_v, s1_v) if j % 2 == 0 else (s1_v, s0_v)
                out, top = step(h, now, top, h + 1 if j < GROUP - 1 else None, later)
                o_v[GROUP // 2 * i + j // 2, :, (j % 2) * HEAD : (j % 2 + 1) * HEAD] = out
            return 0

        lax.fori_loop(0, HEADS // GROUP, body, 0)

    def remote(src, dst, ss, rs, dev):
        return pltpu.make_async_remote_copy(src_ref=src, dst_ref=dst, send_sem=ss, recv_sem=rs, device_id=dev,
                                            device_id_type=pl.DeviceIdType.MESH)

    mine = pl.multiple_of(core * HALF, HALF)
    theirs = pl.multiple_of((1 - core) * HALF, HALF)

    def columns(b, s):
        width = D // parts(b)
        return pl.ds(s * width, width)

    def pair_copy(b, s):
        cols = columns(b, s)
        return remote(pair_send.at[b, :, cols], pair_recv.at[b, :, cols], pair_ss.at[b, s], pair_rs.at[b, s], partner)

    def rs_copy(b, s, k):
        cols = columns(b, s)
        return remote(rs_send.at[b, pl.ds(other(k) * PART, PART), cols], rs_recv.at[b, k - 1, :, cols],
                      rs_ss.at[b, s, k - 1], rs_rs.at[b, s, k - 1], peers[k - 1])

    def ag_copy(b, s, k):
        here = y_ref.at[pl.ds(pl.multiple_of(b * QB + core * HALF + chip * PART, PART), PART), columns(b, s)]
        return remote(here, here, ag_ss.at[b, s, k - 1], ag_rs.at[b, s, k - 1], peers[k - 1])

    def fw_copy(b, s):
        here = y_ref.at[pl.ds(pl.multiple_of(b * QB + core * HALF, HALF), HALF), columns(b, s)]
        return remote(here, here, fw_ss.at[b, s], fw_rs.at[b, s], partner)

    def term(b, rows):
        return sum(dot(o_v[i, rows, :], wo_v[pl.ds(i * 256, 256), :]) for i in range(PAIRS))

    def output(b):
        if b < NB - 1:
            whole = term(b, slice(None))
            if b % 2 == 1:
                normed((b + 1) // 2)
            acc_v[b % 2] = whole
            pair_send[b] = acc_v[b % 2, pl.ds(theirs, HALF), :].astype(BF16)
            pair_copy(b, 0).start()
        else:
            pair_send[b] = term(b, pl.ds(theirs, HALF)).astype(BF16)
            for s in range(parts(b)):
                pair_copy(b, s).start()
            acc_v[b % 2, pl.ds(mine, HALF), :] = term(b, pl.ds(mine, HALF))

    def chip_sum(b, s):
        cols = columns(b, s)
        pair_copy(b, s).wait_recv()
        rs_send[b, :, cols] = (acc_v[b % 2, pl.ds(mine, HALF), cols] + pair_recv[b, :, cols].astype(F32)).astype(BF16)
        for k in FAR_FIRST:
            rs_copy(b, s, k).start()
        part = pl.multiple_of(chip * PART, PART)
        own_v[b, :, cols] = acc_v[b % 2, pl.ds(mine + part, PART), cols] + pair_recv[b, pl.ds(part, PART), cols].astype(F32)

    def finish(b, s):
        cols = columns(b, s)
        total = own_v[b, :, cols]
        for k in range(1, CHIPS):
            rs_copy(b, s, k).wait_recv()
        for k in range(1, CHIPS):
            total = total + rs_recv[b, k - 1, :, cols].astype(F32)
        rows = pl.ds(pl.multiple_of(b * QB + core * HALF + chip * PART, PART), PART)
        y_ref[rows, cols] = (x_v[rows, cols].astype(F32) + total).astype(BF16)
        for k in FAR_FIRST:
            ag_copy(b, s, k).start()

    def forward(b, s):
        for k in range(1, CHIPS):
            ag_copy(b, s, k).wait_recv()
        fw_copy(b, s).start()

    plan = Plan()

    def stages(due):
        for stage, b, s in due:
            (chip_sum, finish, forward)[stage](b, s)

    normed(0)
    for b in range(NB):
        if b % 2 == 0:
            stages(plan.due())
            hooks = {}
            for c in range(1, PAIRS):
                plan.clock += 0.95
                if due := plan.due():
                    hooks[c] = due
            project(b // 2, hooks)
            plan.clock += 0.95
        stages(plan.due())
        hooks = {}
        for i in range(1, HEADS // GROUP):
            plan.clock += ATTENTION[b] * GROUP / HEADS
            if due := plan.due():
                hooks[i] = due
        attention(b, hooks)
        plan.clock += ATTENTION[b] * GROUP / HEADS
        stages(plan.due())
        if b == 0:
            loads["wo"].wait()
            pl.semaphore_wait(barrier, CHIPS)
        output(b)
        plan.clock += 0.8
        plan.send(0, b, 0, -0.4 if b == NB - 1 else 0)
        for s in range(1, parts(b)):
            plan.send(0, b, s, 0.2)
    stages(plan.due(rest=True))
    for b in range(NB):
        for s in range(parts(b)):
            fw_copy(b, s).wait_recv()
            pair_copy(b, s).wait_send()
            for k in range(1, CHIPS):
                rs_copy(b, s, k).wait_send()
                ag_copy(b, s, k).wait_send()
            fw_copy(b, s).wait_send()


def solution(mesh):
    near, far = rotary_tables()

    def step(x, gain, wq, wk, wv, wo):
        vmem, anywhere = pl.BlockSpec(memory_space=pltpu.VMEM), pl.BlockSpec(memory_space=pltpu.HBM)
        dma = pltpu.SemaphoreType.DMA
        return pl.pallas_call(
            kernel,
            out_shape=pltpu.VMEM((ROWS, D), BF16),
            in_specs=[anywhere, vmem, anywhere, vmem, anywhere, anywhere, anywhere, anywhere],
            out_specs=vmem,
            scratch_shapes=[
                pltpu.VMEM((ROWS, D), BF16),
                pltpu.VMEM((2, PB, HEAD), F32),
                pltpu.VMEM((PAIRS, D, 256), BF16),
                pltpu.VMEM((PAIRS, D, 256), BF16),
                pltpu.VMEM((PAIRS, D, 256), BF16),
                pltpu.VMEM((D, D), BF16),
                pltpu.VMEM((PB, D), BF16),
                pltpu.VMEM((PB, HEAD), F32),
                pltpu.VMEM((PB, HEAD), F32),
                pltpu.VMEM((HEADS, ROWS, HEAD), BF16),
                pltpu.VMEM((HEADS, ROWS, HEAD), BF16),
                pltpu.VMEM((HEADS, WIDE, ROWS), BF16),
                pltpu.VMEM((ROWS, QB), F32),
                pltpu.VMEM((ROWS, QB), F32),
                pltpu.VMEM((PAIRS, QB, 256), BF16),
                pltpu.VMEM((2, QB, D), F32),
                pltpu.VMEM((NB, HALF, D), BF16),
                pltpu.VMEM((NB, HALF, D), BF16),
                pltpu.VMEM((NB, HALF, D), BF16),
                pltpu.VMEM((NB, CHIPS - 1, PART, D), BF16),
                pltpu.VMEM((NB, PART, D), F32),
                dma((18,)), dma((NB, SPLIT)), dma((NB, SPLIT)), *[dma((NB, SPLIT, CHIPS - 1))] * 4, dma((NB, SPLIT)), dma((NB, SPLIT)),
            ],
            compiler_params=pltpu.CompilerParams(collective_id=0, has_side_effects=True, vmem_limit_bytes=56 * 2**20),
            cost_estimate=pl.CostEstimate(flops=26 * 10**9, transcendentals=20 * 10**6, bytes_accessed=20 * 2**20),
        )(x, gain, jnp.asarray(near), jnp.asarray(far), wq, wk, wv, wo)

    tokens, columns = P("dp", None), P(None, "tp")
    return jax.shard_map(
        step,
        mesh=mesh,
        in_specs=(tokens, P(None), columns, columns, columns, P("tp", None)),
        out_specs=tokens,
        check_vma=False,
    )
```
